32 devices in a mesh: seq: 8 (over z, x), tp: 4 (over y, core).
Axes of the slice: x: 2, y: 2, z: 4, core: 2. Of those that a mesh axis runs over, the one named last changes fastest.
Arguments:
- prompt_keys: bfloat16 [8, 16384, 512], P(None, 'seq', 'tp'), may hold values from -6 to 16
- prompt_values: bfloat16 [8, 16384, 512], P(None, 'seq', 'tp'), may hold values from -6 to 6
- keep_mask: int32 [8, 128, 4], P(None, 'seq', 'tp'), may hold values from 0 to 1, as said below
- owner_sequence: int32 [8], replicated, may hold values from 0 to 7, each once
- step_queries: bfloat16 [8, 16, 4, 1024], P('seq', None, 'tp'), may hold values from -15 to 26
- new_keys: bfloat16 [8, 16, 512], P('seq', None, 'tp'), may hold values from -12 to 12
- new_values: bfloat16 [8, 16, 512], P('seq', None, 'tp'), may hold values from -6 to 6
Outputs:
- attended: bfloat16 [8, 16, 4, 1024], P('seq', None, 'tp')
The draws below stay inside these ranges and needn't reach their ends.
Inputs may be any that keep to these rules, and one draw needn't show every extreme that they name: `keep_mask`: the last block of every sequence is kept for every head; every sequence and head keeps between 32 and 96 blocks.
All inputs are finite; a program needn't handle non-finite values.
Results may differ from the reference program's by a relative error of at most 0.009.
The reference program's roundings to bfloat16 on the way count: a program that leaves them out, or rounds other values in their place, can miss the bound.
Values may be sent and summed in bfloat16 or wider, within the bound.
No kernel may reach another device: no remote copies, remote signals or barrier semaphores. Data moves between devices by JAX's collectives and lax.ppermute only.
A program may use at most 128 MiB of HBM per device.

```python
import math
import jax
import jax.numpy as jnp
from jax import lax

DH = 128
KVH = 4
QG = 8
BLOCK = 128
STEPS = 16
LEN = 16384
SEQS = 8
NB = 128
KEEP = 96


def draw_keep_mask(key, part):
    count_key, score_key = jax.random.split(jax.random.fold_in(key, 11))
    counts = jax.random.randint(count_key, (SEQS, KVH), NB // 4, KEEP + 1)
    counts = counts.at[0, 0].set(KEEP).at[SEQS - 1, KVH - 1].set(NB // 4)
    block_index = jnp.arange(NB).astype(jnp.int32)
    scores = jax.random.randint(score_key, (SEQS, NB, KVH), 0, 4 * NB) + 2 * block_index[None, :, None]
    scores = jnp.where(block_index[None, :, None] == NB - 1, 10 * NB, scores)
    scores = scores * NB + block_index[None, :, None]
    ordering = jnp.argsort(-scores, axis=1, stable=True)
    ranking = jnp.argsort(ordering, axis=1, stable=True)
    return (ranking < counts[:, None, :]).astype(jnp.int32)


def draw_prompt_keys(key, part):
    shape_all = (SEQS, LEN, KVH * DH)
    normal_part = jnp.clip(jax.random.normal(jax.random.fold_in(key, 21), shape_all, jnp.float32), -6.0, 6.0)
    return normal_part.astype(jnp.bfloat16)


def draw_step_queries(key, part):
    shape_all = (SEQS, STEPS, KVH, QG * DH)
    normal_part = jnp.clip(2.5 * jax.random.normal(jax.random.fold_in(key, 31), shape_all, jnp.float32), -15.0, 15.0)
    return normal_part.astype(jnp.bfloat16)


def levels(stream_key, dims, shards, smallest, top_value):
    def one(dim, parts):
        draws = jax.random.uniform(jax.random.fold_in(jax.random.fold_in(stream_key, 6), dim), (parts,), jnp.float32, smallest / len(shards), top_value / len(shards))
        return jnp.repeat(jnp.exp(draws), dims[dim] // parts).reshape((-1,) + (1,) * (len(dims) - dim - 1))

    factor_of = one(*shards[0])
    for cut in shards[1:]:
        factor_of = factor_of * one(*cut)
    return factor_of


def noise(stream_key, extent, deviation, most, cuts=(), held_as=jnp.bfloat16):
    values = deviation * jax.random.normal(stream_key, extent, jnp.float32)
    if cuts:
        values = values * levels(stream_key, extent, cuts, -0.22, 0.18)
    return jnp.clip(values, -most, most).astype(held_as)


def setup_inputs(seed: int = 0) -> dict:
    key_list = jax.random.split(jax.random.key(seed), 8)
    prompt_keys = draw_prompt_keys(jax.random.fold_in(key_list[7], 71), 0)
    prompt_values = noise(key_list[1], (SEQS, LEN, KVH * DH), 1.0, 6.0, ((1, 8), (2, 4)))
    keep_mask = draw_keep_mask(jax.random.fold_in(key_list[7], 71), 0)
    owner_sequence = jax.random.permutation(key_list[3], SEQS).astype(jnp.int32)
    step_queries = draw_step_queries(jax.random.fold_in(key_list[7], 71), 0)
    new_keys = noise(key_list[5], (SEQS, STEPS, KVH * DH), 2.0, 12.0, ((0, 8), (2, 4)))
    new_values = noise(key_list[6], (SEQS, STEPS, KVH * DH), 1.0, 6.0, ((0, 8), (2, 4)))
    return dict(prompt_keys=prompt_keys, prompt_values=prompt_values, keep_mask=keep_mask, owner_sequence=owner_sequence, step_queries=step_queries, new_keys=new_keys, new_values=new_values)


floor_score = -1e+30

def frequencies(half_width):
    position_index = jnp.arange(half_width).astype(jnp.float32)
    base_rate = jnp.exp(position_index * (-2.0 / (2 * half_width)) * math.log(500000.0))
    wavelength = 2.0 * math.pi / base_rate
    smooth = (8192.0 / wavelength - 1.0) / 3.0
    blended = (1.0 - smooth) * base_rate / 8.0 + smooth * base_rate
    return jnp.where(wavelength < 2048.0, base_rate, jnp.where(wavelength > 8192.0, base_rate / 8.0, blended))

def rotate(vector, offset):
    half_width = vector.shape[-1] // 2
    angles = offset.astype(jnp.float32)[..., None] * frequencies(half_width)
    cosine = jnp.cos(angles)
    sine_part = jnp.sin(angles)
    lower_half = vector[..., :half_width]
    upper_half = vector[..., half_width:]
    return jnp.concatenate([lower_half * cosine - upper_half * sine_part, upper_half * cosine + lower_half * sine_part], axis=-1)

def select_blocks(mask_column):
    running = jnp.cumsum(mask_column).astype(jnp.int32)
    slot_index = jnp.arange(KEEP).astype(jnp.int32)
    chosen = lax.optimization_barrier(jnp.sum((running[None, :] <= slot_index[:, None]).astype(jnp.int32), axis=1)).astype(jnp.int32)
    chosen = jnp.minimum(chosen, mask_column.shape[0] - 1).astype(jnp.int32)
    live_slots = slot_index < running[-1]
    return (chosen, live_slots, ((slot_index - chosen) * BLOCK).astype(jnp.int32))

def attend(query_rows, cached_keys, cached_values, live_tokens, fresh_keys, fresh_values, groups):
    score_scale = 1.0 / math.sqrt(query_rows.shape[-1])
    older = jnp.dot(query_rows, cached_keys.T, preferred_element_type=jnp.float32) * score_scale
    older = jnp.where(live_tokens[None, :], older, floor_score)
    new_scores = jnp.dot(query_rows, fresh_keys.T, preferred_element_type=jnp.float32) * score_scale
    row_step = jnp.arange(query_rows.shape[0]) // groups
    causal = row_step[:, None] >= jnp.arange(fresh_keys.shape[0])[None, :]
    new_scores = jnp.where(causal, new_scores, floor_score)
    highest = jnp.maximum(lax.optimization_barrier(jnp.max(older, axis=1)), lax.optimization_barrier(jnp.max(new_scores, axis=1)))
    older_weight = jnp.where(live_tokens[None, :], jnp.exp(older - highest[:, None]), 0.0)
    newer_weight = jnp.where(causal, jnp.exp(new_scores - highest[:, None]), 0.0)
    row_total = lax.optimization_barrier(jnp.sum(older_weight, axis=1)) + lax.optimization_barrier(jnp.sum(newer_weight, axis=1))
    result = jnp.dot((older_weight / row_total[:, None]).astype(jnp.bfloat16), cached_values, preferred_element_type=jnp.float32)
    result = result + jnp.dot((newer_weight / row_total[:, None]).astype(jnp.bfloat16), fresh_values, preferred_element_type=jnp.float32)
    return result

def reference(prompt_keys, prompt_values, keep_mask, owner_sequence, step_queries, new_keys, new_values):

    def one_owner(owner_rank):
        sequence = owner_sequence[owner_rank]
        mask_rows = keep_mask[sequence]
        counts = lax.optimization_barrier(jnp.sum(mask_rows, axis=0)).astype(jnp.int32)
        first_position = (jnp.max(counts) * BLOCK).astype(jnp.int32)
        positions = first_position + jnp.arange(STEPS).astype(jnp.int32)
        key_blocks = prompt_keys[sequence].reshape(NB, BLOCK, KVH, DH)
        value_blocks = prompt_values[sequence].reshape(NB, BLOCK, KVH, DH)
        query_all = step_queries[owner_rank].reshape(STEPS, KVH, QG, DH)
        fresh_all = new_keys[owner_rank].reshape(STEPS, KVH, DH)
        fresh_vals = new_values[owner_rank].reshape(STEPS, KVH, DH)
        outputs = []
        for head_index in range(KVH):
            chosen, live_slots, offset = select_blocks(mask_rows[:, head_index])
            picked = jnp.take(key_blocks[:, :, head_index], chosen, axis=0)
            turned = rotate(picked.astype(jnp.float32), offset[:, None]).astype(jnp.bfloat16).reshape(KEEP * BLOCK, DH)
            kept_values = jnp.take(value_blocks[:, :, head_index], chosen, axis=0).reshape(KEEP * BLOCK, DH)
            live_tokens = jnp.repeat(live_slots, BLOCK)
            query_rows = rotate(query_all[:, head_index].astype(jnp.float32), positions[:, None]).astype(jnp.bfloat16).reshape(STEPS * QG, DH)
            fresh_turned = rotate(fresh_all[:, head_index].astype(jnp.float32), positions).astype(jnp.bfloat16)
            result = attend(query_rows, turned, kept_values, live_tokens, fresh_turned, fresh_vals[:, head_index], QG)
            outputs.append(result.reshape(STEPS, QG * DH))
        return jnp.stack(outputs, axis=1).astype(jnp.bfloat16)
    return lax.map(one_owner, jnp.arange(SEQS).astype(jnp.int32))
```

```python
import functools
import math

import jax
import jax.numpy as jnp
from jax import lax
from jax.experimental import pallas as pl
from jax.experimental.pallas import tpu as pltpu
from jax.sharding import PartitionSpec as P

BF = jnp.bfloat16
F32 = jnp.float32
EXTRA = 8
floor_score = -1e30
HIGH = lax.Precision.HIGHEST


def frequencies(half_width):
    position_index = jnp.arange(half_width).astype(F32)
    base_rate = jnp.exp(position_index * (-2.0 / (2 * half_width)) * math.log(500000.0))
    wavelength = 2.0 * math.pi / base_rate
    smooth = (8192.0 / wavelength - 1.0) / 3.0
    blended = (1.0 - smooth) * base_rate / 8.0 + smooth * base_rate
    return jnp.where(
        wavelength < 2048.0, base_rate, jnp.where(wavelength > 8192.0, base_rate / 8.0, blended)
    )


def turn_table(positions, width):
    half = width // 2
    angles = positions.astype(F32)[:, None] * frequencies(half)
    cosine, sine = jnp.cos(angles), jnp.sin(angles)
    return jnp.concatenate([cosine, cosine, -sine, sine], axis=1)


def turned(x, cosine, sine):
    return x * cosine + pltpu.roll(x, x.shape[-1] // 2, x.ndim - 1) * sine


def pack_kernel(groups, width, query_ref, near_ref, far_ref, out_ref):
    steps = query_ref.shape[0]
    rows = groups * steps
    parts = [query_ref[:, g * width : (g + 1) * width] for g in range(groups)]
    near = near_ref[...]
    far = far_ref[...]
    counts = jnp.concatenate([near[0:2], far[0:2], near[4:8]], axis=0).astype(BF)
    for target in range(out_ref.shape[0]):
        for g in range(groups):
            out_ref[target, g * steps : (g + 1) * steps, :] = parts[g]
        out_ref[target, rows : rows + EXTRA, :] = counts


def attend_kernel(
    sizes,
    owner_ref,
    keep_ref,
    rank_ref,
    base_ref,
    table_ref,
    step_ref,
    got_ref,
    key_ref,
    value_ref,
    out_ref,
    own_ref,
    cos_k,
    sin_k,
    cos_q,
    sin_q,
    score_ref,
):
    owners, blocks, block, groups, steps, width, heads, chunk = sizes
    rows = groups * steps
    me = rank_ref[0]
    lanes = owners * blocks
    before = jnp.zeros((1, lanes), F32)
    total = jnp.zeros((heads, lanes), F32)
    for i in range(owners):
        piece = got_ref[i, rows : rows + EXTRA, :].astype(F32)
        total = total + piece[0:heads]
        before = before + jnp.where(i < me, piece[0:1], 0.0)
    longest = jnp.max(total, axis=0, keepdims=True)
    dropped = base_ref[0:1, :] - before
    entry = lax.broadcasted_iota(jnp.int32, (table_ref.shape[0], lanes), 0).astype(F32)
    pick_k = (entry == dropped).astype(F32)
    pick_q = (entry == longest).astype(F32)
    dims = (((0,), (0,)), ((), ()))
    for pick, cos_to, sin_to in ((pick_k, cos_k, sin_k), (pick_q, cos_q, sin_q)):
        found = lax.dot_general(
            pick, table_ref[...], dims, precision=HIGH, preferred_element_type=F32
        )
        cos_to[...] = found[:, 0:width]
        sin_to[...] = found[:, width:]
    step_cos, step_sin = step_ref[:, 0:width], step_ref[:, width:]
    factor = math.log2(math.e) / math.sqrt(width)
    lane = lax.broadcasted_iota(jnp.int32, (rows, width), 1)

    def query_turn(s):
        cos0 = cos_q[pl.ds(s * blocks, 1), :]
        sin0 = sin_q[pl.ds(s * blocks, 1), :]
        return cos0 * step_cos - sin0 * step_sin, sin0 * step_cos + cos0 * step_sin

    own_cos, own_sin = query_turn(owner_ref[me])
    own_ref[:, 0:width] = own_cos
    own_ref[:, width:] = own_sin

    @pl.loop(0, owners)
    def _(o):
        s = owner_ref[o]
        cos_now, sin_now = query_turn(s)
        query = got_ref[o, 0:rows, :].astype(F32).reshape(groups, steps, width)
        swapped = pltpu.roll(query.reshape(rows, width), width // 2, 1)
        query = query * cos_now[None] + swapped.reshape(groups, steps, width) * sin_now[None]
        query = query.reshape(rows, width).astype(BF)
        best = jnp.full((rows, width), floor_score, F32)
        per = chunk // block
        for c in range(blocks // per):
            keys = []
            for j in range(per):
                b = c * per + j
                cosine = cos_k[pl.ds(s * blocks + b, 1), :]
                sine = sin_k[pl.ds(s * blocks + b, 1), :]
                x = key_ref[s, b * block : (b + 1) * block, :].astype(F32)
                keys.append(turned(x, cosine, -sine).astype(BF))
            scores = lax.dot_general(
                query,
                jnp.concatenate(keys, axis=0),
                (((1,), (1,)), ((), ())),
                preferred_element_type=F32,
            )
            for j in range(per):
                b = c * per + j
                bias = jnp.where(keep_ref[s * blocks + b] > 0, 0.0, floor_score)
                piece = scores[:, j * block : (j + 1) * block] + bias
                score_ref[:, b * block : (b + 1) * block] = piece
                best = jnp.maximum(best, piece)
        shift = (jnp.max(best, axis=1, keepdims=True) * factor).astype(BF).astype(F32)
        sums = jnp.zeros((rows, block), F32)
        result = jnp.zeros((rows, width), F32)
        for c in range(blocks // per):
            weights = []
            for j in range(per):
                b = c * per + j
                w = jnp.exp2(score_ref[:, b * block : (b + 1) * block] * factor - shift)
                sums = sums + w
                weights.append(w.astype(BF))
            result = result + jnp.dot(
                jnp.concatenate(weights, axis=1),
                value_ref[s, c * chunk : (c + 1) * chunk, :],
                preferred_element_type=F32,
            )
        mass = jnp.sum(sums, axis=1, keepdims=True)
        high = mass.astype(BF).astype(F32)
        notes = jnp.where(lane == 0, shift, jnp.where(lane == 1, high, mass - high))
        out_ref[o, 0:rows, :] = result.astype(BF)
        out_ref[o, rows : rows + EXTRA, :] = notes.T[0:EXTRA].astype(BF)


def fresh_kernel(groups, width, query_ref, own_ref, key_ref, value_ref, out_ref, note_ref):
    steps = query_ref.shape[0]
    rows = groups * steps
    cosine, sine = own_ref[:, 0:width], own_ref[:, width:]
    query = jnp.concatenate(
        [
            turned(query_ref[:, g * width : (g + 1) * width].astype(F32), cosine, sine)
            for g in range(groups)
        ],
        axis=0,
    ).astype(BF)
    fresh = turned(key_ref[...].astype(F32), cosine, sine).astype(BF)
    scores = lax.dot_general(
        query, fresh, (((1,), (1,)), ((), ())), preferred_element_type=F32
    )
    factor = math.log2(math.e) / math.sqrt(width)
    step = lax.rem(lax.broadcasted_iota(jnp.int32, (rows, steps), 0), steps)
    other = lax.broadcasted_iota(jnp.int32, (rows, steps), 1)
    scores = jnp.where(other <= step, scores * factor, floor_score)
    shift = jnp.max(scores, axis=1, keepdims=True)
    weights = jnp.exp2(scores - shift)
    mass = jnp.sum(weights, axis=1, keepdims=True)
    out_ref[...] = jnp.dot(weights.astype(BF), value_ref[...], preferred_element_type=F32)
    lane = lax.broadcasted_iota(jnp.int32, (rows, width), 1)
    note_ref[...] = jnp.where(lane == 0, shift, mass).T[0:EXTRA]


def merge_kernel(groups, steps, got_ref, fresh_ref, note_ref, out_ref):
    owners = got_ref.shape[0]
    width = got_ref.shape[2]
    rows = groups * steps
    shifts = [note_ref[0:1, :]]
    masses = [note_ref[1:2, :]]
    for i in range(owners):
        piece = got_ref[i, rows : rows + EXTRA, :].astype(F32)
        shifts.append(piece[0:1])
        masses.append(piece[1:2] + piece[2:3])
    top = functools.reduce(jnp.maximum, shifts)
    scales = [jnp.exp2(x - top) for x in shifts]
    mass = sum(a * b for a, b in zip(scales, masses))
    scales = [x / mass for x in scales]
    columns = []
    for first in range(0, owners + 1, rows):
        some = scales[first : first + rows]
        pad = jnp.zeros((rows - len(some), rows), F32)
        columns.append(jnp.concatenate(some + [pad], axis=0).T)
    result = fresh_ref[...] * columns[0][:, 0:1]
    for i in range(owners):
        k = i + 1
        result = result + got_ref[i, 0:rows, :].astype(F32) * columns[k // rows][
            :, k % rows : k % rows + 1
        ]
    result = result.astype(BF)
    for g in range(groups):
        out_ref[:, g * width : (g + 1) * width] = result[g * steps : (g + 1) * steps, :]


VMEM = pl.BlockSpec(memory_space=pltpu.VMEM)
SMEM = pl.BlockSpec(memory_space=pltpu.SMEM)


def shards(
    prompt_keys, prompt_values, keep_mask, owner_sequence, step_queries, new_keys, new_values
):
    sequences, tokens_here, width = prompt_keys.shape
    blocks = keep_mask.shape[1]
    block = tokens_here // blocks
    owners = lax.axis_size("seq")
    heads = lax.axis_size("tp")
    rank = lax.axis_index("seq")
    steps = step_queries.shape[1]
    groups = step_queries.shape[3] // width
    rows = groups * steps
    lanes = sequences * blocks
    query = step_queries.reshape(steps, groups * width)
    fresh_keys = new_keys.reshape(steps, width)
    fresh_values = new_values.reshape(steps, width)

    mask = keep_mask.reshape(sequences, blocks)
    count = jnp.sum(mask, axis=1).astype(F32)
    slot = jnp.sum(
        jnp.where(jnp.arange(blocks)[None, :, None] > jnp.arange(blocks)[None, None, :],
                  mask[:, None, :], 0), axis=2)
    base = (rank * blocks + jnp.arange(blocks)[None, :] - slot).astype(F32).reshape(1, lanes)
    base = jnp.broadcast_to(base, (EXTRA, lanes))
    own = jnp.repeat(count, blocks).reshape(1, lanes)
    own = jnp.broadcast_to(own, (EXTRA, lanes))
    other = lax.ppermute(own, "tp", [(i, i ^ 1) for i in range(heads)])
    row = lax.broadcasted_iota(jnp.int32, (EXTRA, lanes), 0)
    near = jnp.where(row == 0, own, jnp.where(row == 1, other, 0.0))
    far = lax.ppermute(near, "tp", [(i, i ^ 2) for i in range(heads)])

    payload = pl.pallas_call(
        functools.partial(pack_kernel, groups, width),
        out_shape=jax.ShapeDtypeStruct((owners, rows + EXTRA, width), BF),
        in_specs=[VMEM] * 3,
        out_specs=VMEM,
        name="pack",
    )(query, near, far)
    got = lax.all_to_all(payload, "seq", split_axis=0, concat_axis=0, tiled=True)

    table = turn_table(jnp.arange(owners * blocks) * block, width)
    step_table = turn_table(jnp.arange(steps), width)
    sizes = (owners, blocks, block, groups, steps, width, heads, min(4, blocks) * block)
    partial, own_turn = pl.pallas_call(
        functools.partial(attend_kernel, sizes),
        out_shape=(
            jax.ShapeDtypeStruct((owners, rows + EXTRA, width), BF),
            jax.ShapeDtypeStruct((steps, 2 * width), F32),
        ),
        in_specs=[SMEM, SMEM, SMEM] + [VMEM] * 6,
        out_specs=(VMEM, VMEM),
        scratch_shapes=[
            pltpu.VMEM((lanes, width), F32),
            pltpu.VMEM((lanes, width), F32),
            pltpu.VMEM((lanes, width), F32),
            pltpu.VMEM((lanes, width), F32),
            pltpu.VMEM((rows, tokens_here), F32),
        ],
        compiler_params=pltpu.CompilerParams(vmem_limit_bytes=40 * 1024 * 1024),
        name="attend",
    )(
        owner_sequence,
        mask.reshape(lanes),
        rank.reshape(1).astype(jnp.int32),
        base,
        table,
        step_table,
        got,
        prompt_keys,
        prompt_values,
    )
    back = lax.all_to_all(partial, "seq", split_axis=0, concat_axis=0, tiled=True)
    fresh, notes = pl.pallas_call(
        functools.partial(fresh_kernel, groups, width),
        out_shape=(
            jax.ShapeDtypeStruct((rows, width), F32),
            jax.ShapeDtypeStruct((EXTRA, rows), F32),
        ),
        in_specs=[VMEM] * 4,
        out_specs=(VMEM, VMEM),
        cost_estimate=pl.CostEstimate(
            flops=4 * rows * steps * width, bytes_accessed=4 * rows * width, transcendentals=0
        ),
        name="fresh",
    )(query, own_turn, fresh_keys, fresh_values)
    merged = pl.pallas_call(
        functools.partial(merge_kernel, groups, steps),
        out_shape=jax.ShapeDtypeStruct((steps, groups * width), BF),
        in_specs=[VMEM] * 3,
        out_specs=VMEM,
        name="merge",
    )(back, fresh, notes)
    return merged.reshape(1, steps, 1, groups * width)


def solution(mesh):
    in_specs = (
        P(None, "seq", "tp"),
        P(None, "seq", "tp"),
        P(None, "seq", "tp"),
        P(),
        P("seq", None, "tp", None),
        P("seq", None, "tp"),
        P("seq", None, "tp"),
    )
    out_specs = P("seq", None, "tp", None)
    return jax.shard_map(shards, mesh=mesh, in_specs=in_specs, out_specs=out_specs, check_vma=False)
```

```python
import functools
import math

import jax
import jax.numpy as jnp
from jax import lax
from jax.experimental import pallas as pl
from jax.experimental.pallas import tpu as pltpu
from jax.sharding import PartitionSpec as P

BF = jnp.bfloat16
F32 = jnp.float32
EXTRA = 8
floor_score = -1e30
HIGH = lax.Precision.HIGHEST


def frequencies(half_width):
    position_index = jnp.arange(half_width).astype(F32)
    base_rate = jnp.exp(position_index * (-2.0 / (2 * half_width)) * math.log(500000.0))
    wavelength = 2.0 * math.pi / base_rate
    smooth = (8192.0 / wavelength - 1.0) / 3.0
    blended = (1.0 - smooth) * base_rate / 8.0 + smooth * base_rate
    return jnp.where(
        wavelength < 2048.0, base_rate, jnp.where(wavelength > 8192.0, base_rate / 8.0, blended)
    )


def turn_table(positions, width):
    half = width // 2
    angles = positions.astype(F32)[:, None] * frequencies(half)
    cosine, sine = jnp.cos(angles), jnp.sin(angles)
    return jnp.concatenate([cosine, cosine, -sine, sine], axis=1)


def iota(shape, axis):
    return lax.broadcasted_iota(jnp.int32, shape, axis)


def turned(x, cosine, sine):
    return x * cosine + pltpu.roll(x, x.shape[-1] // 2, x.ndim - 1) * sine


def count_kernel(keep_ref, count_ref, base_ref):
    sequences, _, blocks = keep_ref.shape
    lanes = sequences * blocks
    me = lax.axis_index("seq")
    keep = keep_ref[...].reshape(sequences, blocks).astype(F32)
    spread = lax.rem(iota((blocks, lanes), 1), blocks) == iota((blocks, lanes), 0)
    wide = jnp.dot(keep, spread.astype(F32), preferred_element_type=F32)
    mine = iota((sequences, lanes), 1) // blocks == iota((sequences, lanes), 0)
    flat = jnp.sum(jnp.where(mine, wide, 0.0), axis=0, keepdims=True)
    flat = jnp.broadcast_to(flat, (EXTRA, lanes))
    row, col = iota((lanes, lanes), 0), iota((lanes, lanes), 1)
    same = row // blocks == col // blocks
    count_ref[...] = jnp.dot(flat, same.astype(F32), preferred_element_type=F32)
    earlier = jnp.dot(flat, (same & (row < col)).astype(F32), preferred_element_type=F32)
    block = (lax.rem(iota((EXTRA, lanes), 1), blocks) + me * blocks).astype(F32)
    base_ref[...] = jnp.where(iota((EXTRA, lanes), 0) == 0, block - earlier, flat)


def pack_kernel(groups, width, query_ref, *refs):
    out_ref = refs[-1]
    steps = query_ref.shape[0]
    rows = groups * steps
    parts = [query_ref[:, g * width : (g + 1) * width] for g in range(groups)]
    counts = [ref[0:1, :] for ref in refs[:-1]]
    fill = refs[0][len(counts) : EXTRA, :]
    counts = jnp.concatenate(counts + [fill], axis=0).astype(BF)
    for target in range(out_ref.shape[0]):
        for g in range(groups):
            out_ref[target, g * steps : (g + 1) * steps, :] = parts[g]
        out_ref[target, rows : rows + EXTRA, :] = counts


def attend_kernel(
    sizes,
    owner_hbm,
    base_ref,
    table_ref,
    step_ref,
    got_ref,
    key_hbm,
    value_hbm,
    out_ref,
    own_ref,
    cos_k,
    sin_k,
    cos_q,
    sin_q,
    bias,
    score_ref,
    key_ref,
    value_ref,
    owner_ref,
    owner_sem,
    key_sem,
    value_sem,
):
    owners, blocks, block, groups, steps, width, heads, chunk = sizes
    rows = groups * steps
    me = lax.axis_index("seq")
    lanes = owners * blocks
    fetch_owner = pltpu.make_async_copy(owner_hbm, owner_ref, owner_sem)
    fetch_owner.start()

    def fetch(s):
        return (
            pltpu.make_async_copy(key_hbm.at[s], key_ref.at[s], key_sem.at[s]),
            pltpu.make_async_copy(value_hbm.at[s], value_ref.at[s], value_sem.at[s]),
        )

    @pl.loop(0, owners)
    def _(s):
        for copy in fetch(s):
            copy.start()

    before = jnp.zeros((1, lanes), F32)
    total = jnp.zeros((heads, lanes), F32)
    for i in range(owners):
        piece = got_ref[i, rows : rows + EXTRA, :].astype(F32)
        total = total + piece[0:heads]
        before = before + jnp.where(i < me, piece[0:1], 0.0)
    longest = jnp.max(total, axis=0, keepdims=True)
    dropped = base_ref[0:1, :] - before
    entry = lax.broadcasted_iota(jnp.int32, (table_ref.shape[0], lanes), 0).astype(F32)
    pick_k = (entry == dropped).astype(F32)
    pick_q = (entry == longest).astype(F32)
    dims = (((0,), (0,)), ((), ()))
    for pick, cos_to, sin_to in ((pick_k, cos_k, sin_k), (pick_q, cos_q, sin_q)):
        found = lax.dot_general(
            pick, table_ref[...], dims, precision=HIGH, preferred_element_type=F32
        )
        cos_to[...] = found[:, 0:width]
        sin_to[...] = found[:, width:]
    kept = jnp.broadcast_to(base_ref[1:2, :], (lanes, lanes)).T[:, 0:block]
    bias[...] = jnp.where(kept > 0.5, 0.0, floor_score)
    fetch_owner.wait()
    step_cos, step_sin = step_ref[:, 0:width], step_ref[:, width:]
    factor = math.log2(math.e) / math.sqrt(width)
    lane = lax.broadcasted_iota(jnp.int32, (rows, width), 1)

    def query_turn(s):
        cos0 = cos_q[pl.ds(s * blocks, 1), :]
        sin0 = sin_q[pl.ds(s * blocks, 1), :]
        return cos0 * step_cos - sin0 * step_sin, sin0 * step_cos + cos0 * step_sin

    own_cos, own_sin = query_turn(owner_ref[me])
    own_ref[:, 0:width] = own_cos
    own_ref[:, width:] = own_sin

    @pl.loop(0, owners)
    def _(s):
        o = lax.fori_loop(0, owners, lambda i, at: jnp.where(owner_ref[i] == s, i, at), 0)
        for copy in fetch(s):
            copy.wait()
        cos_now, sin_now = query_turn(s)
        query = got_ref[o, 0:rows, :].astype(F32).reshape(groups, steps, width)
        swapped = pltpu.roll(query.reshape(rows, width), width // 2, 1)
        query = query * cos_now[None] + swapped.reshape(groups, steps, width) * sin_now[None]
        query = query.reshape(rows, width).astype(BF)
        best = jnp.full((rows, width), floor_score, F32)
        per = chunk // block
        for c in range(blocks // per):
            keys = []
            for j in range(per):
                b = c * per + j
                cosine = cos_k[pl.ds(s * blocks + b, 1), :]
                sine = sin_k[pl.ds(s * blocks + b, 1), :]
                x = key_ref[s, b * block : (b + 1) * block, :].astype(F32)
                keys.append(turned(x, cosine, -sine).astype(BF))
            scores = lax.dot_general(
                query,
                jnp.concatenate(keys, axis=0),
                (((1,), (1,)), ((), ())),
                preferred_element_type=F32,
            )
            for j in range(per):
                b = c * per + j
                piece = scores[:, j * block : (j + 1) * block] + bias[pl.ds(s * blocks + b, 1), :]
                score_ref[:, b * block : (b + 1) * block] = piece
                best = jnp.maximum(best, piece)
        shift = (jnp.max(best, axis=1, keepdims=True) * factor).astype(BF).astype(F32)
        sums = jnp.zeros((rows, block), F32)
        result = jnp.zeros((rows, width), F32)
        for c in range(blocks // per):
            weights = []
            for j in range(per):
                b = c * per + j
                w = jnp.exp2(score_ref[:, b * block : (b + 1) * block] * factor - shift)
                sums = sums + w
                weights.append(w.astype(BF))
            result = result + jnp.dot(
                jnp.concatenate(weights, axis=1),
                value_ref[s, c * chunk : (c + 1) * chunk, :],
                preferred_element_type=F32,
            )
        mass = jnp.sum(sums, axis=1, keepdims=True)
        high = mass.astype(BF).astype(F32)
        notes = jnp.where(lane == 0, shift, jnp.where(lane == 1, high, mass - high))
        out_ref[o, 0:rows, :] = result.astype(BF)
        out_ref[o, rows : rows + EXTRA, :] = notes.T[0:EXTRA].astype(BF)


def fresh_kernel(groups, width, query_ref, own_ref, key_ref, value_ref, out_ref, note_ref):
    steps = query_ref.shape[0]
    rows = groups * steps
    cosine, sine = own_ref[:, 0:width], own_ref[:, width:]
    query = jnp.concatenate(
        [
            turned(query_ref[:, g * width : (g + 1) * width].astype(F32), cosine, sine)
            for g in range(groups)
        ],
        axis=0,
    ).astype(BF)
    fresh = turned(key_ref[...].astype(F32), cosine, sine).astype(BF)
    scores = lax.dot_general(
        query, fresh, (((1,), (1,)), ((), ())), preferred_element_type=F32
    )
    factor = math.log2(math.e) / math.sqrt(width)
    step = lax.rem(lax.broadcasted_iota(jnp.int32, (rows, steps), 0), steps)
    other = lax.broadcasted_iota(jnp.int32, (rows, steps), 1)
    scores = jnp.where(other <= step, scores * factor, floor_score)
    shift = jnp.max(scores, axis=1, keepdims=True)
    weights = jnp.exp2(scores - shift)
    mass = jnp.sum(weights, axis=1, keepdims=True)
    out_ref[...] = jnp.dot(weights.astype(BF), value_ref[...], preferred_element_type=F32)
    lane = lax.broadcasted_iota(jnp.int32, (rows, width), 1)
    note_ref[...] = jnp.where(lane == 0, shift, mass).T[0:EXTRA]


def merge_kernel(groups, steps, got_ref, fresh_ref, note_ref, out_ref):
    owners = got_ref.shape[0]
    width = got_ref.shape[2]
    rows = groups * steps
    shifts = [note_ref[0:1, :]]
    masses = [note_ref[1:2, :]]
    for i in range(owners):
        piece = got_ref[i, rows : rows + EXTRA, :].astype(F32)
        shifts.append(piece[0:1])
        masses.append(piece[1:2] + piece[2:3])
    top = functools.reduce(jnp.maximum, shifts)
    scales = [jnp.exp2(x - top) for x in shifts]
    mass = sum(a * b for a, b in zip(scales, masses))
    scales = [x / mass for x in scales]
    columns = []
    for first in range(0, owners + 1, rows):
        some = scales[first : first + rows]
        pad = jnp.zeros((rows - len(some), rows), F32)
        columns.append(jnp.concatenate(some + [pad], axis=0).T)
    result = fresh_ref[...] * columns[0][:, 0:1]
    for i in range(owners):
        k = i + 1
        result = result + got_ref[i, 0:rows, :].astype(F32) * columns[k // rows][
            :, k % rows : k % rows + 1
        ]
    result = result.astype(BF)
    for g in range(groups):
        out_ref[:, g * width : (g + 1) * width] = result[g * steps : (g + 1) * steps, :]


VMEM = pl.BlockSpec(memory_space=pltpu.VMEM)
ANY = pl.BlockSpec(memory_space=pl.ANY)


def shards(
    prompt_keys, prompt_values, keep_mask, owner_sequence, step_queries, new_keys, new_values
):
    sequences, tokens_here, width = prompt_keys.shape
    blocks = keep_mask.shape[1]
    block = tokens_here // blocks
    owners = lax.axis_size("seq")
    heads = lax.axis_size("tp")
    steps = step_queries.shape[1]
    groups = step_queries.shape[3] // width
    rows = groups * steps
    lanes = sequences * blocks
    small = pltpu.CompilerParams(vmem_limit_bytes=8 * 1024 * 1024)
    query = step_queries.reshape(steps, groups * width)
    fresh_keys = new_keys.reshape(steps, width)
    fresh_values = new_values.reshape(steps, width)

    count, base = pl.pallas_call(
        count_kernel,
        out_shape=(jax.ShapeDtypeStruct((EXTRA, lanes), F32),) * 2,
        in_specs=[VMEM],
        out_specs=(VMEM, VMEM),
        compiler_params=small,
        name="count",
    )(keep_mask.transpose(0, 2, 1))
    counts = [count] + [
        lax.ppermute(count, "tp", [(i, i ^ k) for i in range(heads)]) for k in range(1, heads)
    ]
    payload = pl.pallas_call(
        functools.partial(pack_kernel, groups, width),
        out_shape=jax.ShapeDtypeStruct((owners, rows + EXTRA, width), BF),
        in_specs=[VMEM] * (1 + heads),
        out_specs=VMEM,
        compiler_params=small,
        name="pack",
    )(query, *counts)
    got = lax.all_to_all(payload, "seq", split_axis=0, concat_axis=0, tiled=True)

    table = turn_table(jnp.arange(owners * blocks) * block, width)
    step_table = turn_table(jnp.arange(steps), width)
    sizes = (owners, blocks, block, groups, steps, width, heads, min(4, blocks) * block)
    partial, own_turn = pl.pallas_call(
        functools.partial(attend_kernel, sizes),
        out_shape=(
            jax.ShapeDtypeStruct((owners, rows + EXTRA, width), BF),
            jax.ShapeDtypeStruct((steps, 2 * width), F32),
        ),
        in_specs=[ANY] + [VMEM] * 4 + [ANY] * 2,
        out_specs=(VMEM, VMEM),
        scratch_shapes=[
            pltpu.VMEM((lanes, width), F32),
            pltpu.VMEM((lanes, width), F32),
            pltpu.VMEM((lanes, width), F32),
            pltpu.VMEM((lanes, width), F32),
            pltpu.VMEM((lanes, block), F32),
            pltpu.VMEM((rows, tokens_here), F32),
            pltpu.VMEM(prompt_keys.shape, BF),
            pltpu.VMEM(prompt_values.shape, BF),
            pltpu.SMEM((owners,), jnp.int32),
            pltpu.SemaphoreType.DMA,
            pltpu.SemaphoreType.DMA((owners,)),
            pltpu.SemaphoreType.DMA((owners,)),
        ],
        compiler_params=pltpu.CompilerParams(vmem_limit_bytes=24000000),
        name="attend",
    )(
        pltpu.with_memory_space_constraint(owner_sequence, pltpu.HBM),
        base,
        table,
        step_table,
        got,
        pltpu.with_memory_space_constraint(prompt_keys, pltpu.HBM),
        pltpu.with_memory_space_constraint(prompt_values, pltpu.HBM),
    )
    back = lax.all_to_all(partial, "seq", split_axis=0, concat_axis=0, tiled=True)
    fresh, notes = pl.pallas_call(
        functools.partial(fresh_kernel, groups, width),
        out_shape=(
            jax.ShapeDtypeStruct((rows, width), F32),
            jax.ShapeDtypeStruct((EXTRA, rows), F32),
        ),
        in_specs=[VMEM] * 4,
        out_specs=(VMEM, VMEM),
        cost_estimate=pl.CostEstimate(
            flops=4 * rows * steps * width, bytes_accessed=4 * rows * width, transcendentals=0
        ),
        compiler_params=small,
        name="fresh",
    )(query, own_turn, fresh_keys, fresh_values)
    merged = pl.pallas_call(
        functools.partial(merge_kernel, groups, steps),
        out_shape=jax.ShapeDtypeStruct((steps, groups * width), BF),
        in_specs=[VMEM] * 3,
        out_specs=VMEM,
        compiler_params=small,
        name="merge",
    )(back, fresh, notes)
    return merged.reshape(1, steps, 1, groups * width)


def solution(mesh):
    in_specs = (
        P(None, "seq", "tp"),
        P(None, "seq", "tp"),
        P(None, "seq", "tp"),
        P(),
        P("seq", None, "tp", None),
        P("seq", None, "tp"),
        P("seq", None, "tp"),
    )
    out_specs = P("seq", None, "tp", None)
    return jax.shard_map(shards, mesh=mesh, in_specs=in_specs, out_specs=out_specs, check_vma=False)
```

```python
import functools
import math

import jax
import jax.numpy as jnp
from jax import lax
from jax.experimental import pallas as pl
from jax.experimental.pallas import tpu as pltpu
from jax.sharding import PartitionSpec as P

BF = jnp.bfloat16
F32 = jnp.float32
EXTRA = 8
floor_score = -1e30
HIGH = lax.Precision.HIGHEST


def frequencies(half_width):
    position_index = jnp.arange(half_width).astype(F32)
    base_rate = jnp.exp(position_index * (-2.0 / (2 * half_width)) * math.log(500000.0))
    wavelength = 2.0 * math.pi / base_rate
    smooth = (8192.0 / wavelength - 1.0) / 3.0
    blended = (1.0 - smooth) * base_rate / 8.0 + smooth * base_rate
    return jnp.where(
        wavelength < 2048.0, base_rate, jnp.where(wavelength > 8192.0, base_rate / 8.0, blended)
    )


def turn_table(positions, width):
    half = width // 2
    angles = positions.astype(F32)[:, None] * frequencies(half)
    cosine, sine = jnp.cos(angles), jnp.sin(angles)
    return jnp.concatenate([cosine, cosine, -sine, sine], axis=1)


def iota(shape, axis):
    return lax.broadcasted_iota(jnp.int32, shape, axis)


def turned(x, cosine, sine):
    return x * cosine + pltpu.roll(x, x.shape[-1] // 2, x.ndim - 1) * sine


def count_kernel(keep_ref, count_ref, base_ref):
    sequences, _, blocks = keep_ref.shape
    lanes = sequences * blocks
    me = lax.axis_index("seq")
    keep = keep_ref[...].reshape(sequences, blocks).astype(F32)
    spread = lax.rem(iota((blocks, lanes), 1), blocks) == iota((blocks, lanes), 0)
    wide = jnp.dot(keep, spread.astype(F32), preferred_element_type=F32)
    mine = iota((sequences, lanes), 1) // blocks == iota((sequences, lanes), 0)
    flat = jnp.sum(jnp.where(mine, wide, 0.0), axis=0, keepdims=True)
    flat = jnp.broadcast_to(flat, (EXTRA, lanes))
    row, col = iota((lanes, lanes), 0), iota((lanes, lanes), 1)
    same = row // blocks == col // blocks
    count_ref[...] = jnp.dot(flat, same.astype(F32), preferred_element_type=F32)
    earlier = jnp.dot(flat, (same & (row < col)).astype(F32), preferred_element_type=F32)
    block = (lax.rem(iota((EXTRA, lanes), 1), blocks) + me * blocks).astype(F32)
    base_ref[...] = jnp.where(iota((EXTRA, lanes), 0) == 0, block - earlier, flat)


def pack_kernel(query_ref, *refs):
    out_ref = refs[-1]
    rows = query_ref.shape[0]
    query = query_ref[...]
    counts = [ref[0:1, :] for ref in refs[:-1]]
    fill = refs[0][len(counts) : EXTRA, :]
    counts = jnp.concatenate(counts + [fill], axis=0).astype(BF)
    for target in range(out_ref.shape[0]):
        out_ref[target, 0:rows, :] = query
        out_ref[target, rows : rows + EXTRA, :] = counts


def order_kernel(groups, width, query_ref, out_ref):
    steps = query_ref.shape[0]
    for g in range(groups):
        out_ref[g * steps : (g + 1) * steps, :] = query_ref[:, g * width : (g + 1) * width]


def attend_kernel(
    sizes,
    owner_hbm,
    slot_ref,
    count_ref,
    base_ref,
    table_ref,
    step_ref,
    got_ref,
    key_hbm,
    value_hbm,
    out_ref,
    own_ref,
    cos_k,
    sin_k,
    cos_q,
    sin_q,
    score_a,
    score_b,
    best_a,
    best_b,
    key_ref,
    value_ref,
    owner_ref,
    place_ref,
    owner_sem,
    key_sem,
    value_sem,
):
    owners, blocks, block, groups, steps, width, heads, chunk = sizes
    rows = groups * steps
    me = lax.axis_index("seq")
    lanes = owners * blocks
    fetch_owner = pltpu.make_async_copy(owner_hbm, owner_ref, owner_sem)
    fetch_owner.start()

    def fetch(s):
        return (
            pltpu.make_async_copy(key_hbm.at[s], key_ref.at[s], key_sem.at[s]),
            pltpu.make_async_copy(value_hbm.at[s], value_ref.at[s], value_sem.at[s]),
        )

    @pl.loop(0, owners)
    def _(s):
        for copy in fetch(s):
            copy.start()

    before = jnp.zeros((1, lanes), F32)
    total = jnp.zeros((heads, lanes), F32)
    for i in range(owners):
        piece = got_ref[i, rows : rows + EXTRA, :].astype(F32)
        total = total + piece[0:heads]
        before = before + jnp.where(i < me, piece[0:1], 0.0)
    longest = jnp.max(total, axis=0, keepdims=True)
    dropped = base_ref[0:1, :] - before
    entry = lax.broadcasted_iota(jnp.int32, (table_ref.shape[0], lanes), 0).astype(F32)
    pick_k = (entry == dropped).astype(F32)
    pick_q = (entry == longest).astype(F32)
    dims = (((0,), (0,)), ((), ()))
    table = table_ref[...]
    parts = []
    for _ in range(3):
        part = table.astype(BF)
        parts.append(part)
        table = table - part.astype(F32)
    for pick, cos_to, sin_to in ((pick_k, cos_k, sin_k), (pick_q, cos_q, sin_q)):
        pick = pick.T.astype(BF)
        found = sum(jnp.dot(pick, part, preferred_element_type=F32) for part in parts[::-1])
        cos_to[...] = found[:, 0:width]
        sin_to[...] = found[:, width:]
    fetch_owner.wait()
    step_cos, step_sin = step_ref[:, 0:width], step_ref[:, width:]
    factor = math.log2(math.e) / math.sqrt(width)
    lane = lax.broadcasted_iota(jnp.int32, (rows, width), 1)

    def query_turn(s):
        cos0 = cos_q[pl.ds(s * blocks, 1), :]
        sin0 = sin_q[pl.ds(s * blocks, 1), :]
        return cos0 * step_cos - sin0 * step_sin, sin0 * step_cos + cos0 * step_sin

    own_cos, own_sin = query_turn(owner_ref[me])
    own_ref[:, 0:width] = own_cos
    own_ref[:, width:] = own_sin

    per = chunk // block

    @pl.loop(0, owners)
    def _(i):
        place_ref[owner_ref[i]] = i

    def step_over(ahead, fill, behind, drain):
        if ahead is not None:
            cos_now, sin_now = query_turn(ahead)
            query = got_ref[place_ref[ahead], 0:rows, :].astype(F32)
            swapped = pltpu.roll(query, width // 2, 1).reshape(groups, steps, width)
            query = query.reshape(groups, steps, width) * cos_now[None] + swapped * sin_now[None]
            query = query.reshape(rows, width).astype(BF)
            best = jnp.full((rows, block), -jnp.inf, F32)
        if behind is not None:
            scores_in, best_in = drain
            held = count_ref[behind]
            shift = (jnp.max(best_in[...], axis=1, keepdims=True) * factor).astype(BF).astype(F32)
            result = jnp.zeros((rows, 2 * width), F32)
        for c in range(blocks // per):
            slots = range(c * per, (c + 1) * per)
            if ahead is not None:
                scores_out, best_out = fill
                keys = []
                for r in slots:
                    b = slot_ref[ahead * blocks + r]
                    cosine = cos_k[pl.ds(ahead * blocks + b, 1), :]
                    sine = sin_k[pl.ds(ahead * blocks + b, 1), :]
                    x = key_ref[ahead, pl.ds(pl.multiple_of(b * block, block), block), :]
                    keys.append(turned(x.astype(F32), cosine, -sine).astype(BF))
                scores = lax.dot_general(
                    query,
                    jnp.concatenate(keys, axis=0),
                    (((1,), (1,)), ((), ())),
                    preferred_element_type=F32,
                )
                scores_out[:, c * chunk : (c + 1) * chunk] = scores
                for j in range(per):
                    best = jnp.maximum(best, scores[:, j * block : (j + 1) * block])
            if behind is not None:
                weights = jnp.exp2(scores_in[:, c * chunk : (c + 1) * chunk] * factor - shift)
                values = []
                for r in slots:
                    b = slot_ref[behind * blocks + r]
                    live = jnp.where(r < held, 1.0, 0.0).astype(F32)
                    live = jnp.full((block, width), live, F32).astype(BF)
                    v = value_ref[behind, pl.ds(pl.multiple_of(b * block, block), block), :]
                    values.append(jnp.concatenate([v * live, live], axis=1))
                result = result + jnp.dot(
                    weights.astype(BF),
                    jnp.concatenate(values, axis=0),
                    preferred_element_type=F32,
                )
        if ahead is not None:
            best_out[...] = best
        if behind is not None:
            o = place_ref[behind]
            shift = jnp.where(held > 0, shift, floor_score)
            mass = result[:, width:]
            high = mass.astype(BF).astype(F32)
            notes = jnp.where(lane == 0, shift, jnp.where(lane == 1, high, mass - high))
            out_ref[o, 0:rows, :] = result[:, 0:width].astype(BF)
            out_ref[o, rows : rows + EXTRA, :] = notes.T[0:EXTRA].astype(BF)

    even, odd = (score_a, best_a), (score_b, best_b)
    fetch(0)[0].wait()
    step_over(0, even, None, None)

    @pl.loop(0, owners // 2 - 1)
    def _(i):
        fetch(2 * i + 1)[0].wait()
        fetch(2 * i + 2)[0].wait()
        fetch(2 * i)[1].wait()
        fetch(2 * i + 1)[1].wait()
        step_over(2 * i + 1, odd, 2 * i, even)
        step_over(2 * i + 2, even, 2 * i + 1, odd)

    fetch(owners - 1)[0].wait()
    fetch(owners - 2)[1].wait()
    fetch(owners - 1)[1].wait()
    step_over(owners - 1, odd, owners - 2, even)
    step_over(None, None, owners - 1, odd)


def fresh_kernel(groups, width, query_ref, own_ref, key_ref, value_ref, out_ref, note_ref):
    steps = query_ref.shape[0]
    rows = groups * steps
    cosine, sine = own_ref[:, 0:width], own_ref[:, width:]
    query = jnp.concatenate(
        [
            turned(query_ref[:, g * width : (g + 1) * width].astype(F32), cosine, sine)
            for g in range(groups)
        ],
        axis=0,
    ).astype(BF)
    fresh = turned(key_ref[...].astype(F32), cosine, sine).astype(BF)
    scores = lax.dot_general(
        query, fresh, (((1,), (1,)), ((), ())), preferred_element_type=F32
    )
    factor = math.log2(math.e) / math.sqrt(width)
    step = lax.rem(lax.broadcasted_iota(jnp.int32, (rows, steps), 0), steps)
    other = lax.broadcasted_iota(jnp.int32, (rows, steps), 1)
    scores = jnp.where(other <= step, scores * factor, floor_score)
    shift = jnp.max(scores, axis=1, keepdims=True)
    weights = jnp.exp2(scores - shift)
    mass = jnp.sum(weights, axis=1, keepdims=True)
    out_ref[...] = jnp.dot(weights.astype(BF), value_ref[...], preferred_element_type=F32)
    lane = lax.broadcasted_iota(jnp.int32, (rows, width), 1)
    note_ref[...] = jnp.where(lane == 0, shift, mass).T[0:EXTRA]


def merge_kernel(groups, steps, got_ref, fresh_ref, note_ref, out_ref):
    owners = got_ref.shape[0]
    width = got_ref.shape[2]
    rows = groups * steps
    shifts = [note_ref[0:1, :]]
    masses = [note_ref[1:2, :]]
    for i in range(owners):
        piece = got_ref[i, rows : rows + EXTRA, :].astype(F32)
        shifts.append(piece[0:1])
        masses.append(piece[1:2] + piece[2:3])
    top = functools.reduce(jnp.maximum, shifts)
    scales = [jnp.exp2(x - top) for x in shifts]
    mass = sum(a * b for a, b in zip(scales, masses))
    scales = [x / mass for x in scales]
    columns = []
    for first in range(0, owners + 1, rows):
        some = scales[first : first + rows]
        pad = jnp.zeros((rows - len(some), rows), F32)
        columns.append(jnp.concatenate(some + [pad], axis=0).T)
    result = fresh_ref[...] * columns[0][:, 0:1]
    for i in range(owners):
        k = i + 1
        result = result + got_ref[i, 0:rows, :].astype(F32) * columns[k // rows][
            :, k % rows : k % rows + 1
        ]
    result = result.astype(BF)
    for g in range(groups):
        out_ref[:, g * width : (g + 1) * width] = result[g * steps : (g + 1) * steps, :]


VMEM = pl.BlockSpec(memory_space=pltpu.VMEM)
ANY = pl.BlockSpec(memory_space=pl.ANY)
SMEM = pl.BlockSpec(memory_space=pltpu.SMEM)


def attend(sizes, owner, slots, held, base, table, step_table, got, keys, values, **kw):
    owners, blocks, block, groups, steps, width, heads, chunk = sizes
    rows, lanes = groups * steps, owners * blocks
    return pl.pallas_call(
        functools.partial(attend_kernel, sizes, **kw),
        out_shape=(
            jax.ShapeDtypeStruct((owners, rows + EXTRA, width), BF),
            jax.ShapeDtypeStruct((steps, 2 * width), F32),
        ),
        in_specs=[ANY] + [SMEM] * 2 + [VMEM] * 4 + [ANY] * 2,
        out_specs=(VMEM, VMEM),
        scratch_shapes=[
            pltpu.VMEM((lanes, width), F32),
            pltpu.VMEM((lanes, width), F32),
            pltpu.VMEM((lanes, width), F32),
            pltpu.VMEM((lanes, width), F32),
            pltpu.VMEM((rows, blocks * block), F32),
            pltpu.VMEM((rows, blocks * block), F32),
            pltpu.VMEM((rows, block), F32),
            pltpu.VMEM((rows, block), F32),
            pltpu.VMEM(keys.shape, BF),
            pltpu.VMEM(values.shape, BF),
            pltpu.SMEM((owners,), jnp.int32),
            pltpu.SMEM((owners,), jnp.int32),
            pltpu.SemaphoreType.DMA,
            pltpu.SemaphoreType.DMA((owners,)),
            pltpu.SemaphoreType.DMA((owners,)),
        ],
        compiler_params=pltpu.CompilerParams(vmem_limit_bytes=24 * 1024 * 1024),
        name="attend",
    )(
        pltpu.with_memory_space_constraint(owner, pltpu.HBM),
        slots,
        held,
        base,
        table,
        step_table,
        got,
        pltpu.with_memory_space_constraint(keys, pltpu.HBM),
        pltpu.with_memory_space_constraint(values, pltpu.HBM),
    )


def shards(
    prompt_keys, prompt_values, keep_mask, owner_sequence, step_queries, new_keys, new_values
):
    sequences, tokens_here, width = prompt_keys.shape
    blocks = keep_mask.shape[1]
    block = tokens_here // blocks
    owners = lax.axis_size("seq")
    heads = lax.axis_size("tp")
    steps = step_queries.shape[1]
    groups = step_queries.shape[3] // width
    rows = groups * steps
    lanes = sequences * blocks
    small = pltpu.CompilerParams(vmem_limit_bytes=8 * 1024 * 1024)
    query = step_queries.reshape(steps, groups * width)
    fresh_keys = new_keys.reshape(steps, width)
    fresh_values = new_values.reshape(steps, width)

    count, base = pl.pallas_call(
        count_kernel,
        out_shape=(jax.ShapeDtypeStruct((EXTRA, lanes), F32),) * 2,
        in_specs=[VMEM],
        out_specs=(VMEM, VMEM),
        compiler_params=small,
        name="count",
    )(keep_mask.transpose(0, 2, 1))
    counts = [count] + [
        lax.ppermute(count, "tp", [(i, i ^ k) for i in range(heads)]) for k in range(1, heads)
    ]
    ordered = pl.pallas_call(
        functools.partial(order_kernel, groups, width),
        out_shape=jax.ShapeDtypeStruct((rows, width), BF),
        in_specs=[VMEM],
        out_specs=VMEM,
        compiler_params=small,
        cost_estimate=pl.CostEstimate(
            flops=rows * width, bytes_accessed=4 * rows * width, transcendentals=0
        ),
        name="order",
    )(query)
    payload = pl.pallas_call(
        pack_kernel,
        out_shape=jax.ShapeDtypeStruct((owners, rows + EXTRA, width), BF),
        in_specs=[VMEM] * (1 + heads),
        out_specs=VMEM,
        compiler_params=small,
        name="pack",
    )(ordered, *counts)
    got = lax.all_to_all(payload, "seq", split_axis=0, concat_axis=0, tiled=True)

    mask = keep_mask.reshape(sequences, blocks)
    number = jnp.arange(blocks)
    rank = jnp.sum(jnp.where(number[None, :] < number[:, None], mask[:, None, :], 0), axis=2)
    held = jnp.sum(mask, axis=1)
    wanted = jnp.minimum(number[None, :], held[:, None] - 1)
    found = (rank[:, None, :] == wanted[:, :, None]) & (mask[:, None, :] > 0)
    slots = jnp.sum(jnp.where(found, number[None, None, :], 0), axis=2).reshape(lanes)
    table = turn_table(jnp.arange(owners * blocks) * block, width)
    step_table = turn_table(jnp.arange(steps), width)
    sizes = (owners, blocks, block, groups, steps, width, heads, min(4, blocks) * block)
    partial, own_turn = attend(
        sizes, owner_sequence, slots, held, base, table, step_table, got, prompt_keys, prompt_values
    )
    back = lax.all_to_all(partial, "seq", split_axis=0, concat_axis=0, tiled=True)
    fresh, notes = pl.pallas_call(
        functools.partial(fresh_kernel, groups, width),
        out_shape=(
            jax.ShapeDtypeStruct((rows, width), F32),
            jax.ShapeDtypeStruct((EXTRA, rows), F32),
        ),
        in_specs=[VMEM] * 4,
        out_specs=(VMEM, VMEM),
        cost_estimate=pl.CostEstimate(
            flops=4 * rows * steps * width, bytes_accessed=4 * rows * width, transcendentals=0
        ),
        compiler_params=small,
        name="fresh",
    )(query, own_turn, fresh_keys, fresh_values)
    merged = pl.pallas_call(
        functools.partial(merge_kernel, groups, steps),
        out_shape=jax.ShapeDtypeStruct((steps, groups * width), BF),
        in_specs=[VMEM] * 3,
        out_specs=VMEM,
        compiler_params=small,
        name="merge",
    )(back, fresh, notes)
    return merged.reshape(1, steps, 1, groups * width)


def solution(mesh):
    in_specs = (
        P(None, "seq", "tp"),
        P(None, "seq", "tp"),
        P(None, "seq", "tp"),
        P(),
        P("seq", None, "tp", None),
        P("seq", None, "tp"),
        P("seq", None, "tp"),
    )
    out_specs = P("seq", None, "tp", None)
    return jax.shard_map(shards, mesh=mesh, in_specs=in_specs, out_specs=out_specs, check_vma=False)
```

```python
import functools
import math

import jax
import jax.numpy as jnp
from jax import lax
from jax.experimental import pallas as pl
from jax.experimental.pallas import tpu as pltpu
from jax.sharding import PartitionSpec as P

BF = jnp.bfloat16
F32 = jnp.float32
EXTRA = 8
floor_score = -1e30
HIGH = lax.Precision.HIGHEST


def frequencies(half_width):
    position_index = jnp.arange(half_width).astype(F32)
    base_rate = jnp.exp(position_index * (-2.0 / (2 * half_width)) * math.log(500000.0))
    wavelength = 2.0 * math.pi / base_rate
    smooth = (8192.0 / wavelength - 1.0) / 3.0
    blended = (1.0 - smooth) * base_rate / 8.0 + smooth * base_rate
    return jnp.where(
        wavelength < 2048.0, base_rate, jnp.where(wavelength > 8192.0, base_rate / 8.0, blended)
    )


def turn_table(positions, width):
    half = width // 2
    angles = positions.astype(F32)[:, None] * frequencies(half)
    cosine, sine = jnp.cos(angles), jnp.sin(angles)
    return jnp.concatenate([cosine, cosine, -sine, sine], axis=1)


def iota(shape, axis):
    return lax.broadcasted_iota(jnp.int32, shape, axis)


def turned(x, cosine, sine):
    return x * cosine + pltpu.roll(x, x.shape[-1] // 2, x.ndim - 1) * sine


def count_kernel(keep_ref, count_ref, base_ref):
    sequences, _, blocks = keep_ref.shape
    lanes = sequences * blocks
    me = lax.axis_index("seq")
    keep = keep_ref[...].reshape(sequences, blocks).astype(F32)
    spread = lax.rem(iota((blocks, lanes), 1), blocks) == iota((blocks, lanes), 0)
    wide = jnp.dot(keep, spread.astype(F32), preferred_element_type=F32)
    mine = iota((sequences, lanes), 1) // blocks == iota((sequences, lanes), 0)
    flat = jnp.sum(jnp.where(mine, wide, 0.0), axis=0, keepdims=True)
    flat = jnp.broadcast_to(flat, (EXTRA, lanes))
    row, col = iota((lanes, lanes), 0), iota((lanes, lanes), 1)
    same = row // blocks == col // blocks
    count_ref[...] = jnp.dot(flat, same.astype(F32), preferred_element_type=F32)
    earlier = jnp.dot(flat, (same & (row < col)).astype(F32), preferred_element_type=F32)
    block = (lax.rem(iota((EXTRA, lanes), 1), blocks) + me * blocks).astype(F32)
    base_ref[...] = jnp.where(iota((EXTRA, lanes), 0) == 0, block - earlier, flat)


def slot_kernel(blocks, count_ref, base_ref, out_ref):
    lanes = count_ref.shape[1]
    me = lax.axis_index("seq")
    row, col = iota((lanes, lanes), 0), iota((lanes, lanes), 1)
    block = (lax.rem(col, blocks) + me * blocks).astype(F32)
    rank = block - base_ref[0:1, :]
    rank = jnp.where(base_ref[1:2, :] > 0.5, rank, -2.0).T
    held = count_ref[0:1, :]
    wanted = jnp.minimum(lax.rem(col, blocks).astype(F32), held - 1.0)
    found = (row // blocks == col // blocks) & (rank == wanted)
    slots = jnp.sum(jnp.where(found, lax.rem(row, blocks), 0), axis=0, keepdims=True)
    out_ref[0:1, :] = slots
    out_ref[1:2, :] = held.astype(jnp.int32)


def pack_kernel(query_ref, *refs):
    out_ref = refs[-1]
    rows = query_ref.shape[0]
    query = query_ref[...]
    counts = [ref[0:1, :] for ref in refs[:-1]]
    fill = refs[0][len(counts) : EXTRA, :]
    counts = jnp.concatenate(counts + [fill], axis=0).astype(BF)
    for target in range(out_ref.shape[0]):
        out_ref[target, 0:rows, :] = query
        out_ref[target, rows : rows + EXTRA, :] = counts


def order_kernel(groups, width, query_ref, out_ref):
    steps = query_ref.shape[0]
    for g in range(groups):
        out_ref[g * steps : (g + 1) * steps, :] = query_ref[:, g * width : (g + 1) * width]


def attend_kernel(
    sizes,
    owner_hbm,
    slot_ref,
    base_ref,
    table_ref,
    step_ref,
    got_ref,
    key_hbm,
    value_hbm,
    out_ref,
    own_ref,
    cos_k,
    sin_k,
    cos_q,
    sin_q,
    score_a,
    score_b,
    best_a,
    best_b,
    key_ref,
    value_ref,
    owner_ref,
    place_ref,
    owner_sem,
    key_sem,
    value_sem,
):
    owners, blocks, block, groups, steps, width, heads, chunk = sizes
    rows = groups * steps
    me = lax.axis_index("seq")
    lanes = owners * blocks
    fetch_owner = pltpu.make_async_copy(owner_hbm, owner_ref, owner_sem)
    fetch_owner.start()

    def fetch(s):
        return (
            pltpu.make_async_copy(key_hbm.at[s], key_ref.at[s], key_sem.at[s]),
            pltpu.make_async_copy(value_hbm.at[s], value_ref.at[s], value_sem.at[s]),
        )

    @pl.loop(0, owners)
    def _(s):
        for copy in fetch(s):
            copy.start()

    before = jnp.zeros((1, lanes), F32)
    total = jnp.zeros((heads, lanes), F32)
    for i in range(owners):
        piece = got_ref[i, rows : rows + EXTRA, :].astype(F32)
        total = total + piece[0:heads]
        before = before + jnp.where(i < me, piece[0:1], 0.0)
    longest = jnp.max(total, axis=0, keepdims=True)
    dropped = base_ref[0:1, :] - before
    entry = lax.broadcasted_iota(jnp.int32, (table_ref.shape[0], lanes), 0).astype(F32)
    pick_k = (entry == dropped).astype(F32)
    pick_q = (entry == longest).astype(F32)
    dims = (((0,), (0,)), ((), ()))
    table = table_ref[...]
    parts = []
    for _ in range(3):
        part = table.astype(BF)
        parts.append(part)
        table = table - part.astype(F32)
    for pick, cos_to, sin_to in ((pick_k, cos_k, sin_k), (pick_q, cos_q, sin_q)):
        pick = pick.T.astype(BF)
        found = sum(jnp.dot(pick, part, preferred_element_type=F32) for part in parts[::-1])
        cos_to[...] = found[:, 0:width]
        sin_to[...] = found[:, width:]
    fetch_owner.wait()
    step_cos, step_sin = step_ref[:, 0:width], step_ref[:, width:]
    factor = math.log2(math.e) / math.sqrt(width)
    lane = lax.broadcasted_iota(jnp.int32, (rows, width), 1)

    def query_turn(s):
        cos0 = cos_q[pl.ds(s * blocks, 1), :]
        sin0 = sin_q[pl.ds(s * blocks, 1), :]
        return cos0 * step_cos - sin0 * step_sin, sin0 * step_cos + cos0 * step_sin

    own_cos, own_sin = query_turn(owner_ref[me])
    own_ref[:, 0:width] = own_cos
    own_ref[:, width:] = own_sin

    per = chunk // block

    @pl.loop(0, owners)
    def _(i):
        place_ref[owner_ref[i]] = i

    def step_over(ahead, fill, behind, drain):
        if ahead is not None:
            cos_now, sin_now = query_turn(ahead)
            query = got_ref[place_ref[ahead], 0:rows, :].astype(F32)
            swapped = pltpu.roll(query, width // 2, 1).reshape(groups, steps, width)
            query = query.reshape(groups, steps, width) * cos_now[None] + swapped * sin_now[None]
            query = query.reshape(rows, width).astype(BF)
            best = jnp.full((rows, block), -jnp.inf, F32)
        if behind is not None:
            scores_in, best_in = drain
            held = slot_ref[1, behind * blocks]
            shift = (jnp.max(best_in[...], axis=1, keepdims=True) * factor).astype(BF).astype(F32)
            result = jnp.zeros((rows, 2 * width), F32)
        for c in range(blocks // per):
            slots = range(c * per, (c + 1) * per)
            if ahead is not None:
                scores_out, best_out = fill
                keys = []
                for r in slots:
                    b = slot_ref[0, ahead * blocks + r]
                    cosine = cos_k[pl.ds(ahead * blocks + b, 1), :]
                    sine = sin_k[pl.ds(ahead * blocks + b, 1), :]
                    x = key_ref[ahead, pl.ds(pl.multiple_of(b * block, block), block), :]
                    keys.append(turned(x.astype(F32), cosine, -sine).astype(BF))
                scores = lax.dot_general(
                    query,
                    jnp.concatenate(keys, axis=0),
                    (((1,), (1,)), ((), ())),
                    preferred_element_type=F32,
                )
                scores_out[:, c * chunk : (c + 1) * chunk] = scores
                for j in range(per):
                    best = jnp.maximum(best, scores[:, j * block : (j + 1) * block])
            if behind is not None:
                weights = jnp.exp2(scores_in[:, c * chunk : (c + 1) * chunk] * factor - shift)
                values = []
                for r in slots:
                    b = slot_ref[0, behind * blocks + r]
                    live = jnp.where(r < held, 1.0, 0.0).astype(F32)
                    live = jnp.full((block, width), live, F32).astype(BF)
                    v = value_ref[behind, pl.ds(pl.multiple_of(b * block, block), block), :]
                    values.append(jnp.concatenate([v * live, live], axis=1))
                result = result + jnp.dot(
                    weights.astype(BF),
                    jnp.concatenate(values, axis=0),
                    preferred_element_type=F32,
                )
        if ahead is not None:
            best_out[...] = best
        if behind is not None:
            o = place_ref[behind]
            shift = jnp.where(held > 0, shift, floor_score)
            mass = result[:, width:]
            high = mass.astype(BF).astype(F32)
            notes = jnp.where(lane == 0, shift, jnp.where(lane == 1, high, mass - high))
            out_ref[o, 0:rows, :] = result[:, 0:width].astype(BF)
            out_ref[o, rows : rows + EXTRA, :] = notes.T[0:EXTRA].astype(BF)

    even, odd = (score_a, best_a), (score_b, best_b)
    fetch(0)[0].wait()
    step_over(0, even, None, None)

    @pl.loop(0, owners // 2 - 1)
    def _(i):
        fetch(2 * i + 1)[0].wait()
        fetch(2 * i + 2)[0].wait()
        fetch(2 * i)[1].wait()
        fetch(2 * i + 1)[1].wait()
        step_over(2 * i + 1, odd, 2 * i, even)
        step_over(2 * i + 2, even, 2 * i + 1, odd)

    fetch(owners - 1)[0].wait()
    fetch(owners - 2)[1].wait()
    fetch(owners - 1)[1].wait()
    step_over(owners - 1, odd, owners - 2, even)
    step_over(None, None, owners - 1, odd)


def fresh_kernel(groups, width, query_ref, own_ref, key_ref, value_ref, out_ref, note_ref):
    steps = query_ref.shape[0]
    rows = groups * steps
    cosine, sine = own_ref[:, 0:width], own_ref[:, width:]
    query = jnp.concatenate(
        [
            turned(query_ref[:, g * width : (g + 1) * width].astype(F32), cosine, sine)
            for g in range(groups)
        ],
        axis=0,
    ).astype(BF)
    fresh = turned(key_ref[...].astype(F32), cosine, sine).astype(BF)
    scores = lax.dot_general(
        query, fresh, (((1,), (1,)), ((), ())), preferred_element_type=F32
    )
    factor = math.log2(math.e) / math.sqrt(width)
    step = lax.rem(lax.broadcasted_iota(jnp.int32, (rows, steps), 0), steps)
    other = lax.broadcasted_iota(jnp.int32, (rows, steps), 1)
    scores = jnp.where(other <= step, scores * factor, floor_score)
    shift = jnp.max(scores, axis=1, keepdims=True)
    weights = jnp.exp2(scores - shift)
    mass = jnp.sum(weights, axis=1, keepdims=True)
    out_ref[...] = jnp.dot(weights.astype(BF), value_ref[...], preferred_element_type=F32)
    lane = lax.broadcasted_iota(jnp.int32, (rows, width), 1)
    note_ref[...] = jnp.where(lane == 0, shift, mass).T[0:EXTRA]


def merge_kernel(groups, steps, got_ref, fresh_ref, note_ref, out_ref):
    owners = got_ref.shape[0]
    width = got_ref.shape[2]
    rows = groups * steps
    shifts = [note_ref[0:1, :]]
    masses = [note_ref[1:2, :]]
    for i in range(owners):
        piece = got_ref[i, rows : rows + EXTRA, :].astype(F32)
        shifts.append(piece[0:1])
        masses.append(piece[1:2] + piece[2:3])
    top = functools.reduce(jnp.maximum, shifts)
    scales = [jnp.exp2(x - top) for x in shifts]
    mass = sum(a * b for a, b in zip(scales, masses))
    scales = [x / mass for x in scales]
    columns = []
    for first in range(0, owners + 1, rows):
        some = scales[first : first + rows]
        pad = jnp.zeros((rows - len(some), rows), F32)
        columns.append(jnp.concatenate(some + [pad], axis=0).T)
    result = fresh_ref[...] * columns[0][:, 0:1]
    for i in range(owners):
        k = i + 1
        result = result + got_ref[i, 0:rows, :].astype(F32) * columns[k // rows][
            :, k % rows : k % rows + 1
        ]
    result = result.astype(BF)
    for g in range(groups):
        out_ref[:, g * width : (g + 1) * width] = result[g * steps : (g + 1) * steps, :]


VMEM = pl.BlockSpec(memory_space=pltpu.VMEM)
ANY = pl.BlockSpec(memory_space=pl.ANY)
SMEM = pl.BlockSpec(memory_space=pltpu.SMEM)


def attend(sizes, owner, slots, base, table, step_table, got, keys, values, **kw):
    owners, blocks, block, groups, steps, width, heads, chunk = sizes
    rows, lanes = groups * steps, owners * blocks
    return pl.pallas_call(
        functools.partial(attend_kernel, sizes, **kw),
        out_shape=(
            jax.ShapeDtypeStruct((owners, rows + EXTRA, width), BF),
            jax.ShapeDtypeStruct((steps, 2 * width), F32),
        ),
        in_specs=[ANY] + [SMEM] + [VMEM] * 4 + [ANY] * 2,
        out_specs=(VMEM, VMEM),
        scratch_shapes=[
            pltpu.VMEM((lanes, width), F32),
            pltpu.VMEM((lanes, width), F32),
            pltpu.VMEM((lanes, width), F32),
            pltpu.VMEM((lanes, width), F32),
            pltpu.VMEM((rows, blocks * block), F32),
            pltpu.VMEM((rows, blocks * block), F32),
            pltpu.VMEM((rows, block), F32),
            pltpu.VMEM((rows, block), F32),
            pltpu.VMEM(keys.shape, BF),
            pltpu.VMEM(values.shape, BF),
            pltpu.SMEM((owners,), jnp.int32),
            pltpu.SMEM((owners,), jnp.int32),
            pltpu.SemaphoreType.DMA,
            pltpu.SemaphoreType.DMA((owners,)),
            pltpu.SemaphoreType.DMA((owners,)),
        ],
        compiler_params=pltpu.CompilerParams(vmem_limit_bytes=24 * 1024 * 1024),
        name="attend",
    )(
        pltpu.with_memory_space_constraint(owner, pltpu.HBM),
        slots,
        base,
        table,
        step_table,
        got,
        pltpu.with_memory_space_constraint(keys, pltpu.HBM),
        pltpu.with_memory_space_constraint(values, pltpu.HBM),
    )


def shards(
    prompt_keys, prompt_values, keep_mask, owner_sequence, step_queries, new_keys, new_values
):
    sequences, tokens_here, width = prompt_keys.shape
    blocks = keep_mask.shape[1]
    block = tokens_here // blocks
    owners = lax.axis_size("seq")
    heads = lax.axis_size("tp")
    steps = step_queries.shape[1]
    groups = step_queries.shape[3] // width
    rows = groups * steps
    lanes = sequences * blocks
    small = pltpu.CompilerParams(vmem_limit_bytes=8 * 1024 * 1024)
    query = step_queries.reshape(steps, groups * width)
    fresh_keys = new_keys.reshape(steps, width)
    fresh_values = new_values.reshape(steps, width)

    count, base = pl.pallas_call(
        count_kernel,
        out_shape=(jax.ShapeDtypeStruct((EXTRA, lanes), F32),) * 2,
        in_specs=[VMEM],
        out_specs=(VMEM, VMEM),
        compiler_params=small,
        name="count",
    )(keep_mask.transpose(0, 2, 1))
    counts = [count] + [
        lax.ppermute(count, "tp", [(i, i ^ k) for i in range(heads)]) for k in range(1, heads)
    ]
    ordered = pl.pallas_call(
        functools.partial(order_kernel, groups, width),
        out_shape=jax.ShapeDtypeStruct((rows, width), BF),
        in_specs=[VMEM],
        out_specs=VMEM,
        compiler_params=small,
        cost_estimate=pl.CostEstimate(
            flops=rows * width, bytes_accessed=4 * rows * width, transcendentals=0
        ),
        name="order",
    )(query)
    payload = pl.pallas_call(
        pack_kernel,
        out_shape=jax.ShapeDtypeStruct((owners, rows + EXTRA, width), BF),
        in_specs=[VMEM] * (1 + heads),
        out_specs=VMEM,
        compiler_params=small,
        name="pack",
    )(ordered, *counts)

    payload, count_later, base = lax.optimization_barrier((payload, count, base))
    slots = pl.pallas_call(
        functools.partial(slot_kernel, blocks),
        out_shape=jax.ShapeDtypeStruct((2, lanes), jnp.int32),
        in_specs=[VMEM] * 2,
        out_specs=VMEM,
        compiler_params=small,
        cost_estimate=pl.CostEstimate(
            flops=1000 * lanes * lanes, bytes_accessed=8 * lanes, transcendentals=0
        ),
        name="slots",
    )(count_later, base)
    got = lax.all_to_all(payload, "seq", split_axis=0, concat_axis=0, tiled=True)
    table = turn_table(jnp.arange(owners * blocks) * block, width)
    step_table = turn_table(jnp.arange(steps), width)
    sizes = (owners, blocks, block, groups, steps, width, heads, min(4, blocks) * block)
    partial, own_turn = attend(
        sizes, owner_sequence, slots, base, table, step_table, got, prompt_keys, prompt_values
    )
    back = lax.all_to_all(partial, "seq", split_axis=0, concat_axis=0, tiled=True)
    fresh, notes = pl.pallas_call(
        functools.partial(fresh_kernel, groups, width),
        out_shape=(
            jax.ShapeDtypeStruct((rows, width), F32),
            jax.ShapeDtypeStruct((EXTRA, rows), F32),
        ),
        in_specs=[VMEM] * 4,
        out_specs=(VMEM, VMEM),
        cost_estimate=pl.CostEstimate(
            flops=4 * rows * steps * width, bytes_accessed=4 * rows * width, transcendentals=0
        ),
        compiler_params=small,
        name="fresh",
    )(query, own_turn, fresh_keys, fresh_values)
    merged = pl.pallas_call(
        functools.partial(merge_kernel, groups, steps),
        out_shape=jax.ShapeDtypeStruct((steps, groups * width), BF),
        in_specs=[VMEM] * 3,
        out_specs=VMEM,
        compiler_params=small,
        name="merge",
    )(back, fresh, notes)
    return merged.reshape(1, steps, 1, groups * width)


def solution(mesh):
    in_specs = (
        P(None, "seq", "tp"),
        P(None, "seq", "tp"),
        P(None, "seq", "tp"),
        P(),
        P("seq", None, "tp", None),
        P("seq", None, "tp"),
        P("seq", None, "tp"),
    )
    out_specs = P("seq", None, "tp", None)
    return jax.shard_map(shards, mesh=mesh, in_specs=in_specs, out_specs=out_specs, check_vma=False)
```

```python
import functools
import math

import jax
import jax.numpy as jnp
from jax import lax
from jax.experimental import pallas as pl
from jax.experimental.pallas import tpu as pltpu
from jax.sharding import PartitionSpec as P

BF = jnp.bfloat16
F32 = jnp.float32
EXTRA = 8
floor_score = -1e30
HIGH = lax.Precision.HIGHEST


def frequencies(half_width):
    position_index = jnp.arange(half_width).astype(F32)
    base_rate = jnp.exp(position_index * (-2.0 / (2 * half_width)) * math.log(500000.0))
    wavelength = 2.0 * math.pi / base_rate
    smooth = (8192.0 / wavelength - 1.0) / 3.0
    blended = (1.0 - smooth) * base_rate / 8.0 + smooth * base_rate
    return jnp.where(
        wavelength < 2048.0, base_rate, jnp.where(wavelength > 8192.0, base_rate / 8.0, blended)
    )


def turn_table(positions, width):
    half = width // 2
    angles = positions.astype(F32)[:, None] * frequencies(half)
    cosine, sine = jnp.cos(angles), jnp.sin(angles)
    return jnp.concatenate([cosine, cosine, -sine, sine], axis=1)


def iota(shape, axis):
    return lax.broadcasted_iota(jnp.int32, shape, axis)


def turned(x, cosine, sine):
    return x * cosine + pltpu.roll(x, x.shape[-1] // 2, x.ndim - 1) * sine


def count_kernel(keep_ref, count_ref, base_ref):
    sequences, _, blocks = keep_ref.shape
    lanes = sequences * blocks
    me = lax.axis_index("seq")
    keep = keep_ref[...].reshape(sequences, blocks).astype(F32)
    spread = lax.rem(iota((blocks, lanes), 1), blocks) == iota((blocks, lanes), 0)
    wide = jnp.dot(keep, spread.astype(F32), preferred_element_type=F32)
    mine = iota((sequences, lanes), 1) // blocks == iota((sequences, lanes), 0)
    flat = jnp.sum(jnp.where(mine, wide, 0.0), axis=0, keepdims=True)
    flat = jnp.broadcast_to(flat, (EXTRA, lanes))
    row, col = iota((lanes, lanes), 0), iota((lanes, lanes), 1)
    same = row // blocks == col // blocks
    count_ref[...] = jnp.dot(flat, same.astype(F32), preferred_element_type=F32)
    earlier = jnp.dot(flat, (same & (row < col)).astype(F32), preferred_element_type=F32)
    block = (lax.rem(iota((EXTRA, lanes), 1), blocks) + me * blocks).astype(F32)
    base_ref[...] = jnp.where(iota((EXTRA, lanes), 0) == 0, block - earlier, flat)


def slot_kernel(blocks, count_ref, base_ref, out_ref):
    lanes = count_ref.shape[1]
    me = lax.axis_index("seq")
    row, col = iota((lanes, lanes), 0), iota((lanes, lanes), 1)
    block = (lax.rem(col, blocks) + me * blocks).astype(F32)
    rank = block - base_ref[0:1, :]
    rank = jnp.where(base_ref[1:2, :] > 0.5, rank, -2.0).T
    held = count_ref[0:1, :]
    wanted = jnp.minimum(lax.rem(col, blocks).astype(F32), held - 1.0)
    found = (row // blocks == col // blocks) & (rank == wanted)
    slots = jnp.sum(jnp.where(found, lax.rem(row, blocks), 0), axis=0, keepdims=True)
    out_ref[0:1, :] = slots
    out_ref[1:2, :] = held.astype(jnp.int32)


def pack_kernel(groups, width, query_ref, count_ref, out_ref):
    steps = query_ref.shape[0]
    rows = groups * steps
    parts = [query_ref[:, g * width : (g + 1) * width] for g in range(groups)]
    counts = count_ref[...].astype(BF)
    for target in range(out_ref.shape[0]):
        for g in range(groups):
            out_ref[target, g * steps : (g + 1) * steps, :] = parts[g]
        out_ref[target, rows : rows + EXTRA, :] = counts


def total_kernel(rows, got_ref, out_ref):
    total = jnp.zeros(out_ref.shape, F32)
    for i in range(got_ref.shape[0]):
        total = total + got_ref[i, rows : rows + EXTRA, :].astype(F32)
    out_ref[...] = total


def look_up(pick, table_ref, cos_to, sin_to):
    table = table_ref[...]
    pick = pick.astype(F32).T.astype(BF)
    parts = []
    for _ in range(3):
        part = table.astype(BF)
        parts.append(part)
        table = table - part.astype(F32)
    found = sum(jnp.dot(pick, part, preferred_element_type=F32) for part in parts[::-1])
    width = cos_to.shape[1]
    cos_to[...] = found[:, 0:width]
    sin_to[...] = found[:, width:]


def turn_kernel(sizes, slot_ref, base_ref, table_ref, got_ref, key_hbm, out_ref, cos_k, sin_k, key_ref, key_sem):
    owners, blocks, block, groups, steps, width, heads, chunk = sizes
    rows = groups * steps
    lanes = owners * blocks
    me = lax.axis_index("seq")

    def fetch(s):
        return pltpu.make_async_copy(key_hbm.at[s], key_ref.at[s], key_sem.at[s])

    @pl.loop(0, owners)
    def _(s):
        fetch(s).start()

    before = jnp.zeros((1, lanes), F32)
    for i in range(owners):
        piece = got_ref[i, rows : rows + EXTRA, :].astype(F32)
        before = before + jnp.where(i < me, piece[0:1], 0.0)
    dropped = base_ref[0:1, :] - before
    entry = iota((table_ref.shape[0], lanes), 0).astype(F32)
    look_up(entry == dropped, table_ref, cos_k, sin_k)

    @pl.loop(0, owners)
    def _(s):
        fetch(s).wait()
        for r in range(blocks):
            b = slot_ref[0, s * blocks + r]
            cosine = cos_k[pl.ds(s * blocks + b, 1), :]
            sine = sin_k[pl.ds(s * blocks + b, 1), :]
            x = key_ref[s, pl.ds(pl.multiple_of(b * block, block), block), :].astype(F32)
            out_ref[s, r * block : (r + 1) * block, :] = turned(x, cosine, -sine).astype(BF)


def attend_kernel(
    sizes,
    owner_hbm,
    slot_ref,
    total_ref,
    other_ref,
    another_ref,
    last_ref,
    table_ref,
    step_ref,
    got_ref,
    turned_ref,
    value_hbm,
    out_ref,
    own_ref,
    cos_q,
    sin_q,
    score_a,
    score_b,
    best_a,
    best_b,
    value_ref,
    owner_ref,
    place_ref,
    owner_sem,
    value_sem,
):
    owners, blocks, block, groups, steps, width, heads, chunk = sizes
    rows = groups * steps
    me = lax.axis_index("seq")
    lanes = owners * blocks
    fetch_owner = pltpu.make_async_copy(owner_hbm, owner_ref, owner_sem)
    fetch_owner.start()

    def fetch(s):
        return pltpu.make_async_copy(value_hbm.at[s], value_ref.at[s], value_sem.at[s])

    @pl.loop(0, owners)
    def _(s):
        fetch(s).start()

    longest = total_ref[0:1, :]
    for ref in (other_ref, another_ref, last_ref):
        longest = jnp.maximum(longest, ref[0:1, :])
    entry = iota((table_ref.shape[0], lanes), 0).astype(F32)
    look_up(entry == longest, table_ref, cos_q, sin_q)
    fetch_owner.wait()
    step_cos, step_sin = step_ref[:, 0:width], step_ref[:, width:]
    factor = math.log2(math.e) / math.sqrt(width)
    lane = lax.broadcasted_iota(jnp.int32, (rows, width), 1)

    def query_turn(s):
        cos0 = cos_q[pl.ds(s * blocks, 1), :]
        sin0 = sin_q[pl.ds(s * blocks, 1), :]
        return cos0 * step_cos - sin0 * step_sin, sin0 * step_cos + cos0 * step_sin

    own_cos, own_sin = query_turn(owner_ref[me])
    own_ref[:, 0:width] = own_cos
    own_ref[:, width:] = own_sin

    per = chunk // block

    @pl.loop(0, owners)
    def _(i):
        place_ref[owner_ref[i]] = i

    def step_over(ahead, fill, behind, drain):
        if ahead is not None:
            cos_now, sin_now = query_turn(ahead)
            query = got_ref[place_ref[ahead], 0:rows, :].astype(F32)
            swapped = pltpu.roll(query, width // 2, 1).reshape(groups, steps, width)
            query = query.reshape(groups, steps, width) * cos_now[None] + swapped * sin_now[None]
            query = query.reshape(rows, width).astype(BF)
            best = jnp.full((rows, block), -jnp.inf, F32)
        if behind is not None:
            scores_in, best_in = drain
            held = slot_ref[1, behind * blocks]
            shift = (jnp.max(best_in[...], axis=1, keepdims=True) * factor).astype(BF).astype(F32)
            result = jnp.zeros((rows, 2 * width), F32)
        for c in range(blocks // per):
            slots = range(c * per, (c + 1) * per)
            if ahead is not None:
                scores_out, best_out = fill
                scores = lax.dot_general(
                    query,
                    turned_ref[ahead, c * chunk : (c + 1) * chunk, :],
                    (((1,), (1,)), ((), ())),
                    preferred_element_type=F32,
                )
                scores_out[:, c * chunk : (c + 1) * chunk] = scores
                for j in range(per):
                    best = jnp.maximum(best, scores[:, j * block : (j + 1) * block])
            if behind is not None:
                weights = jnp.exp2(scores_in[:, c * chunk : (c + 1) * chunk] * factor - shift)
                values = []
                for r in slots:
                    b = slot_ref[0, behind * blocks + r]
                    live = jnp.where(r < held, 1.0, 0.0).astype(F32)
                    live = jnp.full((block, width), live, F32).astype(BF)
                    v = value_ref[behind, pl.ds(pl.multiple_of(b * block, block), block), :]
                    values.append(jnp.concatenate([v * live, live], axis=1))
                result = result + jnp.dot(
                    weights.astype(BF),
                    jnp.concatenate(values, axis=0),
                    preferred_element_type=F32,
                )
        if ahead is not None:
            best_out[...] = best
        if behind is not None:
            o = place_ref[behind]
            shift = jnp.where(held > 0, shift, floor_score)
            mass = result[:, width:]
            high = mass.astype(BF).astype(F32)
            notes = jnp.where(lane == 0, shift, jnp.where(lane == 1, high, mass - high))
            out_ref[o, 0:rows, :] = result[:, 0:width].astype(BF)
            out_ref[o, rows : rows + EXTRA, :] = notes.T[0:EXTRA].astype(BF)

    even, odd = (score_a, best_a), (score_b, best_b)
    step_over(0, even, None, None)

    @pl.loop(0, owners // 2 - 1)
    def _(i):
        fetch(2 * i).wait()
        fetch(2 * i + 1).wait()
        step_over(2 * i + 1, odd, 2 * i, even)
        step_over(2 * i + 2, even, 2 * i + 1, odd)

    fetch(owners - 2).wait()
    fetch(owners - 1).wait()
    step_over(owners - 1, odd, owners - 2, even)
    step_over(None, None, owners - 1, odd)


def fresh_kernel(groups, width, query_ref, own_ref, key_ref, value_ref, out_ref, note_ref):
    steps = query_ref.shape[0]
    rows = groups * steps
    cosine, sine = own_ref[:, 0:width], own_ref[:, width:]
    query = jnp.concatenate(
        [
            turned(query_ref[:, g * width : (g + 1) * width].astype(F32), cosine, sine)
            for g in range(groups)
        ],
        axis=0,
    ).astype(BF)
    fresh = turned(key_ref[...].astype(F32), cosine, sine).astype(BF)
    scores = lax.dot_general(
        query, fresh, (((1,), (1,)), ((), ())), preferred_element_type=F32
    )
    factor = math.log2(math.e) / math.sqrt(width)
    step = lax.rem(lax.broadcasted_iota(jnp.int32, (rows, steps), 0), steps)
    other = lax.broadcasted_iota(jnp.int32, (rows, steps), 1)
    scores = jnp.where(other <= step, scores * factor, floor_score)
    shift = jnp.max(scores, axis=1, keepdims=True)
    weights = jnp.exp2(scores - shift)
    mass = jnp.sum(weights, axis=1, keepdims=True)
    out_ref[...] = jnp.dot(weights.astype(BF), value_ref[...], preferred_element_type=F32)
    lane = lax.broadcasted_iota(jnp.int32, (rows, width), 1)
    note_ref[...] = jnp.where(lane == 0, shift, mass).T[0:EXTRA]


def merge_kernel(groups, steps, got_ref, fresh_ref, note_ref, out_ref):
    owners = got_ref.shape[0]
    width = got_ref.shape[2]
    rows = groups * steps
    shifts = [note_ref[0:1, :]]
    masses = [note_ref[1:2, :]]
    for i in range(owners):
        piece = got_ref[i, rows : rows + EXTRA, :].astype(F32)
        shifts.append(piece[0:1])
        masses.append(piece[1:2] + piece[2:3])
    top = functools.reduce(jnp.maximum, shifts)
    scales = [jnp.exp2(x - top) for x in shifts]
    mass = sum(a * b for a, b in zip(scales, masses))
    scales = [x / mass for x in scales]
    columns = []
    for first in range(0, owners + 1, rows):
        some = scales[first : first + rows]
        pad = jnp.zeros((rows - len(some), rows), F32)
        columns.append(jnp.concatenate(some + [pad], axis=0).T)
    result = fresh_ref[...] * columns[0][:, 0:1]
    for i in range(owners):
        k = i + 1
        result = result + got_ref[i, 0:rows, :].astype(F32) * columns[k // rows][
            :, k % rows : k % rows + 1
        ]
    result = result.astype(BF)
    for g in range(groups):
        out_ref[:, g * width : (g + 1) * width] = result[g * steps : (g + 1) * steps, :]


VMEM = pl.BlockSpec(memory_space=pltpu.VMEM)
ANY = pl.BlockSpec(memory_space=pl.ANY)
SMEM = pl.BlockSpec(memory_space=pltpu.SMEM)


def turn(sizes, slots, base, table, got, keys):
    owners, blocks, block, groups, steps, width, heads, chunk = sizes
    lanes = owners * blocks
    return pl.pallas_call(
        functools.partial(turn_kernel, sizes),
        out_shape=jax.ShapeDtypeStruct(keys.shape, BF),
        in_specs=[SMEM] + [VMEM] * 3 + [ANY],
        out_specs=VMEM,
        scratch_shapes=[
            pltpu.VMEM((lanes, width), F32),
            pltpu.VMEM((lanes, width), F32),
            pltpu.VMEM(keys.shape, BF),
            pltpu.SemaphoreType.DMA((owners,)),
        ],
        compiler_params=pltpu.CompilerParams(vmem_limit_bytes=12 * 1024 * 1024),
        cost_estimate=pl.CostEstimate(
            flops=256 * keys.size, bytes_accessed=4 * keys.size, transcendentals=0
        ),
        name="turn",
    )(slots, base, table, got, pltpu.with_memory_space_constraint(keys, pltpu.HBM))


def attend(sizes, owner, slots, totals, table, step_table, got, keys, values):
    owners, blocks, block, groups, steps, width, heads, chunk = sizes
    rows, lanes = groups * steps, owners * blocks
    return pl.pallas_call(
        functools.partial(attend_kernel, sizes),
        out_shape=(
            jax.ShapeDtypeStruct((owners, rows + EXTRA, width), BF),
            jax.ShapeDtypeStruct((steps, 2 * width), F32),
        ),
        in_specs=[ANY] + [SMEM] + [VMEM] * 8 + [ANY],
        out_specs=(VMEM, VMEM),
        scratch_shapes=[
            pltpu.VMEM((lanes, width), F32),
            pltpu.VMEM((lanes, width), F32),
            pltpu.VMEM((rows, blocks * block), F32),
            pltpu.VMEM((rows, blocks * block), F32),
            pltpu.VMEM((rows, block), F32),
            pltpu.VMEM((rows, block), F32),
            pltpu.VMEM(values.shape, BF),
            pltpu.SMEM((owners,), jnp.int32),
            pltpu.SMEM((owners,), jnp.int32),
            pltpu.SemaphoreType.DMA,
            pltpu.SemaphoreType.DMA((owners,)),
        ],
        compiler_params=pltpu.CompilerParams(vmem_limit_bytes=16 * 1024 * 1024),
        name="attend",
    )(
        pltpu.with_memory_space_constraint(owner, pltpu.HBM),
        slots,
        *totals,
        table,
        step_table,
        got,
        keys,
        pltpu.with_memory_space_constraint(values, pltpu.HBM),
    )


def shards(
    prompt_keys, prompt_values, keep_mask, owner_sequence, step_queries, new_keys, new_values
):
    sequences, tokens_here, width = prompt_keys.shape
    blocks = keep_mask.shape[1]
    block = tokens_here // blocks
    owners = lax.axis_size("seq")
    heads = lax.axis_size("tp")
    steps = step_queries.shape[1]
    groups = step_queries.shape[3] // width
    rows = groups * steps
    lanes = sequences * blocks
    small = pltpu.CompilerParams(vmem_limit_bytes=8 * 1024 * 1024)
    query = step_queries.reshape(steps, groups * width)
    fresh_keys = new_keys.reshape(steps, width)
    fresh_values = new_values.reshape(steps, width)

    count, base = pl.pallas_call(
        count_kernel,
        out_shape=(jax.ShapeDtypeStruct((EXTRA, lanes), F32),) * 2,
        in_specs=[VMEM],
        out_specs=(VMEM, VMEM),
        compiler_params=small,
        name="count",
    )(keep_mask.transpose(0, 2, 1))
    payload = pl.pallas_call(
        functools.partial(pack_kernel, groups, width),
        out_shape=jax.ShapeDtypeStruct((owners, rows + EXTRA, width), BF),
        in_specs=[VMEM] * 2,
        out_specs=VMEM,
        compiler_params=small,
        name="pack",
    )(query, count)
    payload, count_later, base = lax.optimization_barrier((payload, count, base))
    slots = pl.pallas_call(
        functools.partial(slot_kernel, blocks),
        out_shape=jax.ShapeDtypeStruct((2, lanes), jnp.int32),
        in_specs=[VMEM] * 2,
        out_specs=VMEM,
        compiler_params=small,
        cost_estimate=pl.CostEstimate(
            flops=1000 * lanes * lanes, bytes_accessed=8 * lanes, transcendentals=0
        ),
        name="slots",
    )(count_later, base)
    got = lax.all_to_all(payload, "seq", split_axis=0, concat_axis=0, tiled=True)

    table = turn_table(jnp.arange(owners * blocks) * block, width)
    step_table = turn_table(jnp.arange(steps), width)
    sizes = (owners, blocks, block, groups, steps, width, heads, min(4, blocks) * block)
    total = pl.pallas_call(
        functools.partial(total_kernel, rows),
        out_shape=jax.ShapeDtypeStruct((EXTRA, lanes), F32),
        in_specs=[VMEM],
        out_specs=VMEM,
        compiler_params=small,
        name="total",
    )(got)
    totals = [total] + [
        lax.ppermute(total, "tp", [(i, i ^ k) for i in range(heads)]) for k in range(1, heads)
    ]
    keys = turn(sizes, slots, base, table, got, prompt_keys)
    partial, own_turn = attend(
        sizes, owner_sequence, slots, totals, table, step_table, got, keys, prompt_values
    )
    back = lax.all_to_all(partial, "seq", split_axis=0, concat_axis=0, tiled=True)
    fresh, notes = pl.pallas_call(
        functools.partial(fresh_kernel, groups, width),
        out_shape=(
            jax.ShapeDtypeStruct((rows, width), F32),
            jax.ShapeDtypeStruct((EXTRA, rows), F32),
        ),
        in_specs=[VMEM] * 4,
        out_specs=(VMEM, VMEM),
        cost_estimate=pl.CostEstimate(
            flops=4 * rows * steps * width, bytes_accessed=4 * rows * width, transcendentals=0
        ),
        compiler_params=small,
        name="fresh",
    )(query, own_turn, fresh_keys, fresh_values)
    merged = pl.pallas_call(
        functools.partial(merge_kernel, groups, steps),
        out_shape=jax.ShapeDtypeStruct((steps, groups * width), BF),
        in_specs=[VMEM] * 3,
        out_specs=VMEM,
        compiler_params=small,
        name="merge",
    )(back, fresh, notes)
    return merged.reshape(1, steps, 1, groups * width)


def solution(mesh):
    in_specs = (
        P(None, "seq", "tp"),
        P(None, "seq", "tp"),
        P(None, "seq", "tp"),
        P(),
        P("seq", None, "tp", None),
        P("seq", None, "tp"),
        P("seq", None, "tp"),
    )
    out_specs = P("seq", None, "tp", None)
    return jax.shard_map(shards, mesh=mesh, in_specs=in_specs, out_specs=out_specs, check_vma=False)
```
